32 devices in a mesh: rep: 2 (over x), ep: 8 (over z, core), fsdp: 2 (over y).
Axes of the slice: x: 2, y: 2, z: 4, core: 2. Of those that a mesh axis runs over, the one named last changes fastest.
Arguments:
- weights: bfloat16 [8, 1024, 7168], P('ep', None, ('rep', 'fsdp')), may hold values from -6 to 6
- offsets: int32 [1], replicated, may hold values from 0 to 7
Outputs:
- codes: bfloat16 [8, 1024, 7168], P('ep', None, 'rep')
- scales: bfloat16 [8, 8, 56], P('ep', None, ('rep', 'fsdp'))
The draws below stay inside these ranges and needn't reach their ends.
Inputs may be any that keep to these rules, and one draw needn't show every extreme that they name: `offsets`: A placement map over the 8 owners.
All inputs are finite; a program needn't handle non-finite values. Where the reference program divides by a largest or mean magnitude, that divisor is 1e-20 or more.
Results may differ from the reference program's by a relative error of at most 0.001.
Values may be sent and summed in bfloat16 or wider, within the bound.
A program may use at most 128 MiB of HBM per device.

```python
import jax
import jax.numpy as jnp
from jax import lax

D = 7168
EXP_DEV = 1
ROWS = 1024
BLOCK = 128
EXPERTS = 8
N_EP = 8


def block_scale(own_key, dims, split, low, high):
    factor_of = 1.0
    for dim, blocks in split:
        heights = jax.random.uniform(jax.random.fold_in(jax.random.fold_in(own_key, 6), dim), (blocks,), jnp.float32, low / len(split), high / len(split))
        factor_of = factor_of * jnp.repeat(jnp.exp(heights), dims[dim] // blocks).reshape((-1,) + (1,) * (len(dims) - 1 - dim))
    return factor_of


def normal_values(own_key, shape, deviation, limit, shards=(), held_as=jnp.bfloat16):
    result = deviation * jax.random.normal(own_key, shape, jnp.float32)
    if shards:
        result = result * block_scale(own_key, shape, shards, -0.22, 0.18)
    return jnp.clip(result, -limit, limit).astype(held_as)


def setup_inputs(seed: int = 0) -> dict:
    seeds = jax.random.split(jax.random.key(seed), 3)
    weights = normal_values(seeds[0], (EXPERTS, ROWS, D), 1.0, 6.0, ((0, 8), (2, 4)))
    offsets = jax.random.randint(seeds[1], (EXP_DEV,), 0, N_EP).astype(jnp.int32)
    return {"weights": weights, "offsets": offsets}


epsilon = 1e-6


def reference(weights, offsets):
    owners = jnp.arange(N_EP, dtype=jnp.int32)[:, None]
    places = jnp.arange(EXP_DEV, dtype=jnp.int32)[None, :]
    source = (((owners - offsets.astype(jnp.int32)[None, :]) % N_EP) * EXP_DEV + places).reshape(-1).astype(jnp.int32)

    def one_expert(index):
        matrix = weights[index].astype(jnp.float32)
        blocks = matrix.reshape(ROWS // BLOCK, BLOCK, D // BLOCK, BLOCK)
        amax = jnp.max(jnp.abs(blocks), axis=(1, 3))
        scaled = (blocks / (amax[:, None, :, None] + epsilon)).reshape(ROWS, D).astype(jnp.bfloat16)
        return scaled, amax.astype(jnp.bfloat16)

    codes, scales = lax.map(one_expert, source)
    return codes, scales
```

```python
import functools

import jax
import jax.numpy as jnp
from jax import lax
from jax.experimental import pallas as pl
from jax.experimental.pallas import tpu as pltpu
from jax.sharding import PartitionSpec as P

BLOCK = 128
CHUNK = 32
epsilon = 1e-06
MESH = pl.DeviceIdType.MESH


def move_kernel(shift, owners, replicas, w_ref, out_ref, send_sem, recv_sem, fsend_sem, frecv_sem, local_sem):
    me = lax.axis_index("ep")
    side = lax.axis_index("fsdp")
    rows = w_ref.shape[0]
    chunks = rows // CHUNK
    target = lax.rem(me + shift, owners)
    source = lax.rem(me + owners - shift, owners)
    partners = [lax.rem(side + k, replicas) for k in range(1, replicas)]

    barrier = pltpu.get_barrier_semaphore()
    if shift:
        pl.semaphore_signal(barrier, inc=1, device_id={"ep": source}, device_id_type=MESH)
    for partner in partners:
        pl.semaphore_signal(barrier, inc=1, device_id={"fsdp": partner}, device_id_type=MESH)
    pl.semaphore_wait(barrier, len(partners) + (1 if shift else 0))

    def span(c):
        return pl.ds(pl.multiple_of(c * CHUNK, CHUNK), CHUNK)

    def first(c):
        return pltpu.make_async_remote_copy(
            src_ref=w_ref.at[span(c)],
            dst_ref=out_ref.at[side, span(c)],
            send_sem=send_sem.at[c],
            recv_sem=recv_sem.at[c],
            device_id={"ep": target},
            device_id_type=MESH,
        )

    def second(c, k):
        src = out_ref.at[side, span(c)] if shift else w_ref.at[span(c)]
        return pltpu.make_async_remote_copy(
            src_ref=src,
            dst_ref=out_ref.at[side, span(c)],
            send_sem=fsend_sem.at[k, c],
            recv_sem=frecv_sem.at[k, c],
            device_id={"fsdp": partners[k]},
            device_id_type=MESH,
        )

    def local(c):
        return pltpu.make_async_copy(w_ref.at[span(c)], out_ref.at[side, span(c)], local_sem.at[c])

    @pl.loop(0, chunks)
    def _(c):
        if shift:
            first(c).start()
        else:
            local(c).start()

    @pl.loop(0, chunks)
    def _(c):
        if shift:
            first(c).wait_recv()
        for k in range(replicas - 1):
            second(c, k).start()

    @pl.loop(0, chunks)
    def _(c):
        if shift:
            first(c).wait_send()
        else:
            local(c).wait()
        for k in range(replicas - 1):
            second(c, k).wait()


def move(shift, owners, replicas, weights):
    rows, columns = weights.shape
    chunks = rows // CHUNK
    return pl.pallas_call(
        functools.partial(move_kernel, shift, owners, replicas),
        out_shape=jax.ShapeDtypeStruct((replicas, rows, columns), weights.dtype),
        in_specs=[pl.BlockSpec(memory_space=pl.ANY)],
        out_specs=pl.BlockSpec(memory_space=pl.ANY),
        scratch_shapes=[
            pltpu.SemaphoreType.DMA((chunks,)),
            pltpu.SemaphoreType.DMA((chunks,)),
            pltpu.SemaphoreType.DMA((max(replicas - 1, 1), chunks)),
            pltpu.SemaphoreType.DMA((max(replicas - 1, 1), chunks)),
            pltpu.SemaphoreType.DMA((chunks,)),
        ],
        compiler_params=pltpu.CompilerParams(
            collective_id=shift, has_side_effects=True
        ),
        name=f"move_{shift}",
    )(weights)


def scale_kernel(x_ref, codes_ref, amax_ref):
    columns = x_ref.shape[2]
    for b in range(columns // BLOCK):
        at = slice(b * BLOCK, (b + 1) * BLOCK)
        x = x_ref[0, :, at].astype(jnp.float32)
        amax = jnp.max(jnp.abs(x))
        codes_ref[:, at] = (x / (amax + epsilon)).astype(codes_ref.dtype)
        amax_ref[0, 0, 0, :, at] = jnp.full((1, BLOCK), amax, jnp.float32)


def scale(moved):
    replicas, rows, columns = moved.shape
    steps = rows // BLOCK
    return pl.pallas_call(
        scale_kernel,
        grid=(replicas, steps),
        out_shape=(
            jax.ShapeDtypeStruct((rows, replicas * columns), moved.dtype),
            jax.ShapeDtypeStruct((replicas, steps, 1, 1, columns), jnp.float32),
        ),
        in_specs=[pl.BlockSpec((1, BLOCK, columns), lambda r, i: (r, i, 0))],
        out_specs=(
            pl.BlockSpec((BLOCK, columns), lambda r, i: (i, r)),
            pl.BlockSpec((1, 1, 1, 1, columns), lambda r, i: (r, i, 0, 0, 0)),
        ),
        name="scale",
    )(moved)


def on_device(weights, offsets):
    owners, replicas = lax.axis_size("ep"), lax.axis_size("fsdp")
    side = lax.axis_index("fsdp")
    codes, scales = [], []
    for k in range(weights.shape[0]):
        branches = [
            functools.partial(move, shift, owners, replicas) for shift in range(owners)
        ]
        moved = lax.switch(offsets[k], branches, weights[k])
        code, amax = scale(moved)
        codes.append(code)
        own = lax.dynamic_index_in_dim(amax, side, 0, keepdims=False)
        scales.append(own[:, 0, 0, ::BLOCK].astype(jnp.bfloat16))
    return jnp.stack(codes), jnp.stack(scales)


def solution(mesh):
    in_specs = (P("ep", None, ("rep", "fsdp")), P())
    out_specs = (P("ep", None, "rep"), P("ep", None, ("rep", "fsdp")))
    return jax.shard_map(
        on_device, mesh=mesh, in_specs=in_specs, out_specs=out_specs, check_vma=False
    )
```

```python
import functools

import jax
import jax.numpy as jnp
from jax import lax
from jax.experimental import pallas as pl
from jax.experimental.pallas import tpu as pltpu
from jax.sharding import PartitionSpec as P

BLOCK = 128
CHUNK = 32
LANES = 128
SPARE = 8 * 2**20
epsilon = 1e-06
MESH = pl.DeviceIdType.MESH


def move_kernel(
    shift, owners, replicas, w_ref, codes_ref, scales_ref,
    land_ref, amax_ref, send_sem, recv_sem, fsend_sem, frecv_sem, local_sem,
):
    me = lax.axis_index("ep")
    side = lax.axis_index("fsdp")
    rows, columns = w_ref.shape
    steps, per = rows // BLOCK, BLOCK // CHUNK
    chunks = rows // CHUNK
    target = lax.rem(me + shift, owners)
    source = lax.rem(me + owners - shift, owners)
    partners = [lax.rem(side + k, replicas) for k in range(1, replicas)]

    barrier = pltpu.get_barrier_semaphore()
    if shift:
        pl.semaphore_signal(barrier, inc=1, device_id={"ep": source}, device_id_type=MESH)
    for partner in partners:
        pl.semaphore_signal(barrier, inc=1, device_id={"fsdp": partner}, device_id_type=MESH)

    def span(c):
        return pl.ds(pl.multiple_of(c * CHUNK, CHUNK), CHUNK)

    def first(c):
        if not shift:
            return pltpu.make_async_copy(w_ref.at[span(c)], land_ref.at[side, span(c)], local_sem.at[c])
        return pltpu.make_async_remote_copy(
            src_ref=w_ref.at[span(c)],
            dst_ref=land_ref.at[side, span(c)],
            send_sem=send_sem.at[c],
            recv_sem=recv_sem.at[c],
            device_id={"ep": target},
            device_id_type=MESH,
        )

    def second(c, k):
        return pltpu.make_async_remote_copy(
            src_ref=land_ref.at[side, span(c)],
            dst_ref=land_ref.at[side, span(c)],
            send_sem=fsend_sem.at[k, c],
            recv_sem=frecv_sem.at[k, c],
            device_id={"fsdp": partners[k]},
            device_id_type=MESH,
        )

    def scaled(r, i, keep):
        at_rows = pl.ds(pl.multiple_of(i * BLOCK, BLOCK), BLOCK)
        lane = lax.broadcasted_iota(jnp.int32, (1, LANES), 1)
        line = jnp.zeros((1, LANES), jnp.float32)
        for b in range(columns // BLOCK):
            at = slice(b * BLOCK, (b + 1) * BLOCK)
            x = land_ref[r, at_rows, at].astype(jnp.float32)
            amax = jnp.max(jnp.max(jnp.abs(x), axis=0, keepdims=True), axis=1, keepdims=True)
            codes_ref[r, at_rows, at] = (x / (amax + epsilon)).astype(codes_ref.dtype)
            if keep:
                line = jnp.where(lane == b, amax, line)
        if keep:
            amax_ref[pl.ds(i, 1), :] = line

    pl.semaphore_wait(barrier, len(partners) + (1 if shift else 0))

    @pl.loop(0, chunks)
    def _(c):
        first(c).start()

    @pl.loop(0, steps + 1)
    def _(i):
        @pl.when(i < steps)
        def _():
            @pl.loop(i * per, i * per + per)
            def _(c):
                if shift:
                    first(c).wait_recv()
                else:
                    first(c).wait()
                for k in range(replicas - 1):
                    second(c, k).start()

            scaled(side, i, True)

        for k in range(replicas - 1):
            other = lax.rem(side + replicas - 1 - k, replicas)

            @pl.when(i >= 1)
            def _():
                @pl.loop((i - 1) * per, i * per)
                def _(c):
                    second(c, k).wait_recv()

                scaled(other, i - 1, False)

    scales_ref[...] = amax_ref[:, : columns // BLOCK].astype(scales_ref.dtype)

    @pl.loop(0, chunks)
    def _(c):
        if shift:
            first(c).wait_send()
        for k in range(replicas - 1):
            second(c, k).wait_send()


def move(shift, owners, replicas, weights):
    rows, columns = weights.shape
    chunks = rows // CHUNK
    steps = rows // BLOCK
    return pl.pallas_call(
        functools.partial(move_kernel, shift, owners, replicas),
        out_shape=(
            pltpu.VMEM((replicas, rows, columns), weights.dtype),
            jax.ShapeDtypeStruct((steps, columns // BLOCK), weights.dtype),
        ),
        in_specs=[pl.BlockSpec(memory_space=pltpu.HBM)],
        out_specs=(
            pl.BlockSpec(memory_space=pltpu.VMEM),
            pl.BlockSpec(memory_space=pltpu.VMEM),
        ),
        scratch_shapes=[
            pltpu.VMEM((replicas, rows, columns), weights.dtype),
            pltpu.VMEM((steps, LANES), jnp.float32),
            pltpu.SemaphoreType.DMA((chunks,)),
            pltpu.SemaphoreType.DMA((chunks,)),
            pltpu.SemaphoreType.DMA((max(replicas - 1, 1), chunks)),
            pltpu.SemaphoreType.DMA((max(replicas - 1, 1), chunks)),
            pltpu.SemaphoreType.DMA((chunks,)),
        ],
        compiler_params=pltpu.CompilerParams(
            collective_id=shift,
            has_side_effects=True,
            vmem_limit_bytes=replicas * rows * columns * weights.dtype.itemsize + SPARE,
        ),
        name=f"move_{shift}",
    )(weights)


def store_kernel(codes_ref, scales_in_ref, out_ref, scales_ref, sem):
    replicas, rows, columns = codes_ref.shape
    parts = rows // BLOCK
    copies = []
    for r in range(replicas):
        for i in range(parts):
            at = pl.ds(i * BLOCK, BLOCK)
            copies.append(
                pltpu.make_async_copy(
                    codes_ref.at[r, at],
                    out_ref.at[at, pl.ds(r * columns, columns)],
                    sem.at[r, i],
                )
            )
    for copy in copies:
        copy.start()
    scales_ref[...] = scales_in_ref[...]
    for copy in copies:
        copy.wait()


def store(codes, scales):
    replicas, rows, columns = codes.shape
    return pl.pallas_call(
        store_kernel,
        out_shape=(
            jax.ShapeDtypeStruct((rows, replicas * columns), codes.dtype),
            jax.ShapeDtypeStruct(scales.shape, scales.dtype),
        ),
        in_specs=[
            pl.BlockSpec(memory_space=pltpu.VMEM),
            pl.BlockSpec(memory_space=pltpu.VMEM),
        ],
        out_specs=(
            pl.BlockSpec(memory_space=pltpu.HBM),
            pl.BlockSpec(memory_space=pltpu.VMEM),
        ),
        scratch_shapes=[pltpu.SemaphoreType.DMA((replicas, rows // BLOCK))],
        compiler_params=pltpu.CompilerParams(vmem_limit_bytes=SPARE),
        name="store",
    )(codes, scales)


def placed(shift, owners, replicas, weights):
    return store(*move(shift, owners, replicas, weights))


def on_device(weights, offsets):
    owners, replicas = lax.axis_size("ep"), lax.axis_size("fsdp")
    codes, scales = [], []
    for k in range(weights.shape[0]):
        branches = [
            functools.partial(placed, shift, owners, replicas) for shift in range(owners)
        ]
        code, scale = lax.switch(offsets[k], branches, weights[k])
        codes.append(code)
        scales.append(scale)
    return jnp.stack(codes), jnp.stack(scales)


def solution(mesh):
    in_specs = (P("ep", None, ("rep", "fsdp")), P())
    out_specs = (P("ep", None, "rep"), P("ep", None, ("rep", "fsdp")))
    return jax.shard_map(
        on_device, mesh=mesh, in_specs=in_specs, out_specs=out_specs, check_vma=False
    )
```

```python
import functools

import jax
import jax.numpy as jnp
from jax import lax
from jax.experimental import pallas as pl
from jax.experimental.pallas import tpu as pltpu
from jax.sharding import PartitionSpec as P

BLOCK = 128
LAG = 4
WIDE = 2
LANES = 128
SPARE = 8 * 2**20
epsilon = 1e-06
MESH = pl.DeviceIdType.MESH


def move_kernel(
    shift, owners, replicas, w_ref, codes_ref, scales_ref,
    stage_ref, land_ref, amax_ref, send_sem, recv_sem, fsend_sem, frecv_sem, local_sem,
):
    me = lax.axis_index("ep")
    side = lax.axis_index("fsdp")
    rows, columns = w_ref.shape
    groups, _, width = stage_ref.shape
    steps = rows // BLOCK
    pieces = groups * steps
    target = lax.rem(me + shift, owners)
    source = lax.rem(me + owners - shift, owners)
    partners = [lax.rem(side + k, replicas) for k in range(1, replicas)]

    staged = [
        pltpu.make_async_copy(
            w_ref.at[:, pl.ds(g * width, width)],
            stage_ref.at[g] if shift else land_ref.at[side, g],
            local_sem.at[g],
        )
        for g in range(groups)
    ]
    for copy in staged:
        copy.start()

    barrier = pltpu.get_barrier_semaphore()
    if shift:
        pl.semaphore_signal(barrier, inc=1, device_id={"ep": source}, device_id_type=MESH)
    for partner in partners:
        pl.semaphore_signal(barrier, inc=1, device_id={"fsdp": partner}, device_id_type=MESH)

    def place(c):
        g, i = lax.div(c, steps), lax.rem(c, steps)
        return g, i, pl.ds(pl.multiple_of(i * BLOCK, BLOCK), BLOCK)

    def first(c):
        g, _, span = place(c)
        return pltpu.make_async_remote_copy(
            src_ref=stage_ref.at[g, span],
            dst_ref=land_ref.at[side, g, span],
            send_sem=send_sem.at[c],
            recv_sem=recv_sem.at[c],
            device_id={"ep": target},
            device_id_type=MESH,
        )

    def second(c, k):
        g, _, span = place(c)
        return pltpu.make_async_remote_copy(
            src_ref=land_ref.at[side, g, span],
            dst_ref=land_ref.at[side, g, span],
            send_sem=fsend_sem.at[k, c],
            recv_sem=frecv_sem.at[k, c],
            device_id={"fsdp": partners[k]},
            device_id_type=MESH,
        )

    def scaled(r, c, keep):
        g, i, span = place(c)
        if keep:
            lane = lax.broadcasted_iota(jnp.int32, (1, LANES), 1)
            line = amax_ref[pl.ds(i, 1), :]
        for b in range(width // BLOCK):
            at = slice(b * BLOCK, (b + 1) * BLOCK)
            x = land_ref[r, g, span, at].astype(jnp.float32)
            amax = jnp.max(jnp.max(jnp.abs(x), axis=0, keepdims=True), axis=1, keepdims=True)
            to = pl.ds(pl.multiple_of(g * width + b * BLOCK, BLOCK), BLOCK)
            codes_ref[r, span, to] = (x / (amax + epsilon)).astype(codes_ref.dtype)
            if keep:
                line = jnp.where(lane == g * (width // BLOCK) + b, amax, line)
        if keep:
            amax_ref[pl.ds(i, 1), :] = line

    amax_ref[...] = jnp.zeros_like(amax_ref)
    pl.semaphore_wait(barrier, len(partners) + (1 if shift else 0))

    for g in range(groups):
        staged[g].wait()

        @pl.loop(g * steps, (g + 1) * steps)
        def _(c):
            if shift:
                first(c).start()
            else:
                for k in range(replicas - 1):
                    second(c, k).start()

    @pl.loop(0, pieces + LAG)
    def _(c):
        @pl.when(c < pieces)
        def _():
            if shift:
                first(c).wait_recv()
                for k in range(replicas - 1):
                    second(c, k).start()
            scaled(side, c, True)

        @pl.when(c >= LAG)
        def _():
            for k in range(replicas - 1):
                second(c - LAG, k).wait_recv()
                scaled(lax.rem(side + replicas - 1 - k, replicas), c - LAG, False)

    scales_ref[...] = amax_ref[:, : columns // BLOCK].astype(scales_ref.dtype)

    @pl.loop(0, pieces)
    def _(c):
        if shift:
            first(c).wait_send()
        for k in range(replicas - 1):
            second(c, k).wait_send()


def move(shift, owners, replicas, weights):
    rows, columns = weights.shape
    steps = rows // BLOCK
    blocks = columns // BLOCK
    groups = blocks // WIDE if blocks % WIDE == 0 else blocks
    pieces = groups * steps
    landing = (groups, rows, columns // groups)
    return pl.pallas_call(
        functools.partial(move_kernel, shift, owners, replicas),
        out_shape=(
            pltpu.VMEM((replicas, rows, columns), weights.dtype),
            jax.ShapeDtypeStruct((steps, columns // BLOCK), weights.dtype),
        ),
        in_specs=[pl.BlockSpec(memory_space=pltpu.HBM)],
        out_specs=(
            pl.BlockSpec(memory_space=pltpu.VMEM),
            pl.BlockSpec(memory_space=pltpu.VMEM),
        ),
        scratch_shapes=[
            pltpu.VMEM(landing, weights.dtype),
            pltpu.VMEM((replicas, *landing), weights.dtype),
            pltpu.VMEM((steps, LANES), jnp.float32),
            pltpu.SemaphoreType.DMA((pieces,)),
            pltpu.SemaphoreType.DMA((pieces,)),
            pltpu.SemaphoreType.DMA((max(replicas - 1, 1), pieces)),
            pltpu.SemaphoreType.DMA((max(replicas - 1, 1), pieces)),
            pltpu.SemaphoreType.DMA((groups,)),
        ],
        compiler_params=pltpu.CompilerParams(
            collective_id=shift,
            has_side_effects=True,
            vmem_limit_bytes=(replicas + 1) * rows * columns * weights.dtype.itemsize + SPARE,
        ),
        name=f"move_{shift}",
    )(weights)


def store_kernel(codes_ref, scales_in_ref, out_ref, scales_ref, sem):
    replicas, rows, columns = codes_ref.shape
    parts = rows // BLOCK
    copies = []
    for r in range(replicas):
        for i in range(parts):
            at = pl.ds(i * BLOCK, BLOCK)
            copies.append(
                pltpu.make_async_copy(
                    codes_ref.at[r, at],
                    out_ref.at[at, pl.ds(r * columns, columns)],
                    sem.at[r, i],
                )
            )
    for copy in copies:
        copy.start()
    scales_ref[...] = scales_in_ref[...]
    for copy in copies:
        copy.wait()


def store(codes, scales):
    replicas, rows, columns = codes.shape
    return pl.pallas_call(
        store_kernel,
        out_shape=(
            jax.ShapeDtypeStruct((rows, replicas * columns), codes.dtype),
            jax.ShapeDtypeStruct(scales.shape, scales.dtype),
        ),
        in_specs=[
            pl.BlockSpec(memory_space=pltpu.VMEM),
            pl.BlockSpec(memory_space=pltpu.VMEM),
        ],
        out_specs=(
            pl.BlockSpec(memory_space=pltpu.HBM),
            pl.BlockSpec(memory_space=pltpu.VMEM),
        ),
        scratch_shapes=[pltpu.SemaphoreType.DMA((replicas, rows // BLOCK))],
        compiler_params=pltpu.CompilerParams(vmem_limit_bytes=SPARE),
        name="store",
    )(codes, scales)


def placed(shift, owners, replicas, weights):
    return store(*move(shift, owners, replicas, weights))


def on_device(weights, offsets):
    owners, replicas = lax.axis_size("ep"), lax.axis_size("fsdp")
    codes, scales = [], []
    for k in range(weights.shape[0]):
        branches = [
            functools.partial(placed, shift, owners, replicas) for shift in range(owners)
        ]
        code, scale = lax.switch(offsets[k], branches, weights[k])
        codes.append(code)
        scales.append(scale)
    return jnp.stack(codes), jnp.stack(scales)


def solution(mesh):
    in_specs = (P("ep", None, ("rep", "fsdp")), P())
    out_specs = (P("ep", None, "rep"), P("ep", None, ("rep", "fsdp")))
    return jax.shard_map(
        on_device, mesh=mesh, in_specs=in_specs, out_specs=out_specs, check_vma=False
    )
```

```python
import functools

import jax
import jax.numpy as jnp
from jax import lax
from jax.experimental import pallas as pl
from jax.experimental.pallas import tpu as pltpu
from jax.sharding import PartitionSpec as P

BLOCK = 128
LAG = 4
WIDE = 2
LANES = 128
SPARE = 8 * 2**20
epsilon = 1e-06
MESH = pl.DeviceIdType.MESH


def move_kernel(
    shift, owners, replicas, w_ref, codes_ref, scales_ref,
    stage_ref, land_ref, amax_ref, send_sem, recv_sem, fsend_sem, frecv_sem, local_sem,
):
    me = lax.axis_index("ep")
    side = lax.axis_index("fsdp")
    rows, columns = w_ref.shape
    groups, _, width = stage_ref.shape
    steps = rows // BLOCK
    pieces = groups * steps
    target = lax.rem(me + shift, owners)
    source = lax.rem(me + owners - shift, owners)
    partners = [lax.rem(side + k, replicas) for k in range(1, replicas)]

    staged = [
        pltpu.make_async_copy(
            w_ref.at[:, pl.ds(g * width, width)],
            stage_ref.at[g] if shift else land_ref.at[side, g],
            local_sem.at[g],
        )
        for g in range(groups)
    ]
    for copy in staged:
        copy.start()

    barrier = pltpu.get_barrier_semaphore()
    if shift:
        pl.semaphore_signal(barrier, inc=1, device_id={"ep": source}, device_id_type=MESH)
    for partner in partners:
        pl.semaphore_signal(barrier, inc=1, device_id={"fsdp": partner}, device_id_type=MESH)

    def place(c):
        g, i = lax.div(c, steps), lax.rem(c, steps)
        return g, i, pl.ds(pl.multiple_of(i * BLOCK, BLOCK), BLOCK)

    def first(c):
        g, _, span = place(c)
        return pltpu.make_async_remote_copy(
            src_ref=stage_ref.at[g, span],
            dst_ref=land_ref.at[side, g, span],
            send_sem=send_sem.at[c],
            recv_sem=recv_sem.at[c],
            device_id={"ep": target},
            device_id_type=MESH,
        )

    def second(c, k):
        g, _, span = place(c)
        return pltpu.make_async_remote_copy(
            src_ref=land_ref.at[side, g, span],
            dst_ref=land_ref.at[side, g, span],
            send_sem=fsend_sem.at[k, c],
            recv_sem=frecv_sem.at[k, c],
            device_id={"fsdp": partners[k]},
            device_id_type=MESH,
        )

    def scaled(r, c, keep):
        g, i, span = place(c)
        if keep:
            lane = lax.broadcasted_iota(jnp.int32, (1, LANES), 1)
            line = amax_ref[pl.ds(i, 1), :]
        for b in range(width // BLOCK):
            at = slice(b * BLOCK, (b + 1) * BLOCK)
            x = land_ref[r, g, span, at].astype(jnp.float32)
            amax = jnp.max(jnp.max(jnp.abs(x), axis=0, keepdims=True), axis=1, keepdims=True)
            to = pl.ds(pl.multiple_of(g * width + b * BLOCK, BLOCK), BLOCK)
            codes_ref[r, span, to] = (x / (amax + epsilon)).astype(codes_ref.dtype)
            if keep:
                line = jnp.where(lane == g * (width // BLOCK) + b, amax, line)
        if keep:
            amax_ref[pl.ds(i, 1), :] = line

    amax_ref[...] = jnp.zeros_like(amax_ref)
    pl.semaphore_wait(barrier, len(partners) + (1 if shift else 0))

    for g in range(groups):
        staged[g].wait()

        @pl.loop(g * steps, (g + 1) * steps)
        def _(c):
            if shift:
                first(c).start()
            else:
                for k in range(replicas - 1):
                    second(c, k).start()

    @pl.loop(0, pieces + LAG)
    def _(c):
        @pl.when(c < pieces)
        def _():
            if shift:
                first(c).wait_recv()
                for k in range(replicas - 1):
                    second(c, k).start()
            scaled(side, c, True)

        @pl.when(c >= LAG)
        def _():
            for k in range(replicas - 1):
                second(c - LAG, k).wait_recv()
                scaled(lax.rem(side + replicas - 1 - k, replicas), c - LAG, False)

    scales_ref[...] = amax_ref[:, : columns // BLOCK].astype(scales_ref.dtype)

    @pl.loop(0, pieces)
    def _(c):
        if shift:
            first(c).wait_send()
        for k in range(replicas - 1):
            second(c, k).wait_send()


def move(shift, owners, replicas, weights):
    rows, columns = weights.shape
    steps = rows // BLOCK
    blocks = columns // BLOCK
    near = min(shift, owners - shift) < 2
    wide = max(WIDE, blocks // WIDE) if near else WIDE
    groups = blocks // wide if blocks % wide == 0 else blocks
    pieces = groups * steps
    landing = (groups, rows, columns // groups)
    return pl.pallas_call(
        functools.partial(move_kernel, shift, owners, replicas),
        out_shape=(
            pltpu.VMEM((replicas, rows, columns), weights.dtype),
            jax.ShapeDtypeStruct((steps, columns // BLOCK), weights.dtype),
        ),
        in_specs=[pl.BlockSpec(memory_space=pltpu.HBM)],
        out_specs=(
            pl.BlockSpec(memory_space=pltpu.VMEM),
            pl.BlockSpec(memory_space=pltpu.VMEM),
        ),
        scratch_shapes=[
            pltpu.VMEM(landing, weights.dtype),
            pltpu.VMEM((replicas, *landing), weights.dtype),
            pltpu.VMEM((steps, LANES), jnp.float32),
            pltpu.SemaphoreType.DMA((pieces,)),
            pltpu.SemaphoreType.DMA((pieces,)),
            pltpu.SemaphoreType.DMA((max(replicas - 1, 1), pieces)),
            pltpu.SemaphoreType.DMA((max(replicas - 1, 1), pieces)),
            pltpu.SemaphoreType.DMA((groups,)),
        ],
        compiler_params=pltpu.CompilerParams(
            collective_id=shift,
            has_side_effects=True,
            vmem_limit_bytes=(replicas + 1) * rows * columns * weights.dtype.itemsize + SPARE,
        ),
        name=f"move_{shift}",
    )(weights)


def store_kernel(codes_ref, scales_in_ref, out_ref, scales_ref, sem, small_sem):
    replicas, rows, columns = codes_ref.shape
    parts = rows // BLOCK
    copies = [pltpu.make_async_copy(scales_in_ref, scales_ref, small_sem.at[0])]
    for r in range(replicas):
        for i in range(parts):
            at = pl.ds(i * BLOCK, BLOCK)
            copies.append(
                pltpu.make_async_copy(
                    codes_ref.at[r, at],
                    out_ref.at[at, pl.ds(r * columns, columns)],
                    sem.at[r, i],
                )
            )
    for copy in copies:
        copy.start()
    for copy in copies:
        copy.wait()


def store(codes, scales):
    replicas, rows, columns = codes.shape
    return pl.pallas_call(
        store_kernel,
        out_shape=(
            jax.ShapeDtypeStruct((rows, replicas * columns), codes.dtype),
            jax.ShapeDtypeStruct(scales.shape, scales.dtype),
        ),
        in_specs=[
            pl.BlockSpec(memory_space=pltpu.VMEM),
            pl.BlockSpec(memory_space=pltpu.VMEM),
        ],
        out_specs=(
            pl.BlockSpec(memory_space=pltpu.HBM),
            pl.BlockSpec(memory_space=pltpu.HBM),
        ),
        scratch_shapes=[
            pltpu.SemaphoreType.DMA((replicas, rows // BLOCK)),
            pltpu.SemaphoreType.DMA((1,)),
        ],
        compiler_params=pltpu.CompilerParams(vmem_limit_bytes=SPARE),
        name="store",
    )(codes, scales)


def placed(shift, owners, replicas, weights):
    return store(*move(shift, owners, replicas, weights))


def on_device(weights, offsets):
    owners, replicas = lax.axis_size("ep"), lax.axis_size("fsdp")
    codes, scales = [], []
    for k in range(weights.shape[0]):
        branches = [
            functools.partial(placed, shift, owners, replicas) for shift in range(owners)
        ]
        code, scale = lax.switch(offsets[k], branches, weights[k])
        codes.append(code)
        scales.append(scale)
    return jnp.stack(codes), jnp.stack(scales)


def solution(mesh):
    in_specs = (P("ep", None, ("rep", "fsdp")), P())
    out_specs = (P("ep", None, "rep"), P("ep", None, ("rep", "fsdp")))
    return jax.shard_map(
        on_device, mesh=mesh, in_specs=in_specs, out_specs=out_specs, check_vma=False
    )
```
